1024 devices in a mesh: sfc: 128 (over x, z), grp: 8 (over y, core).
Axes of the slice: x: 4, y: 4, z: 32, core: 2. Of those that a mesh axis runs over, the one named last changes fastest.
Arguments:
- tracers: float32 [16, 4, 8, 196608], P(None, None, None, ('sfc', 'grp')), may hold values from 0.05 to 60, as said below
- send_counts: int32 [128, 8, 24], P('sfc', 'grp'), may hold values from 1 to 256, 3072 in all within a row
- point_order: int32 [128, 8, 3072], P('sfc', 'grp'), may hold values from 0 to 3071, each once within a row
- depart_elem: int32 [128, 8, 3, 8, 256], P('sfc', 'grp'), may hold values from 0 to 191
- depart_coords: float32 [128, 8, 2, 3, 8, 256], P('sfc', 'grp'), may hold values from -1 to 1
Outputs:
- transported: float32 [16, 4, 8, 196608], P(None, None, None, ('sfc', 'grp'))
The draws below stay inside these ranges and needn't reach their ends.
Inputs may be any that keep to these rules, and one draw needn't show every extreme that they name: `send_counts`: each row lists, for the 24 owner blocks of one device, how many of its arrival points depart from that owner's elements; a row sums to 3072, and its largest entry is exactly 256. `point_order`: each row is a permutation of the device's arrival points. `tracers`: Positive.
All inputs are finite; a program needn't handle non-finite values.
Results may differ from the reference program's by a relative error of at most 0.0003.
Values sent between devices are 32-bit elements; how exact they have to be, the bound alone decides.
A program may use at most 64 MiB of HBM per device.

```python
import math
import jax
import jax.numpy as jnp
import numpy as np
from jax import lax

NODES = 16
TRACERS = 8
LEVELS = 4
E_DEV = 192
SEGMENTS = 128
GROUPS = 8
PEERS = 24
POINTS = 3072
CAP = 256
NE = 196608


def draw_tracers(key, part):
    base = jax.random.uniform(jax.random.fold_in(key, 11), (NODES, LEVELS, TRACERS, NE), jnp.float32)
    magnitude = jax.random.uniform(jax.random.fold_in(key, 12), (LEVELS, TRACERS), jnp.float32, 0.3, 0.8)
    flips = jax.random.randint(jax.random.fold_in(key, 13), (LEVELS, TRACERS), 0, 2)
    slope = jnp.where(flips == 0, -magnitude, magnitude)
    node_line = jnp.arange(NODES, dtype=jnp.int32) // 4
    node_x = jnp.array([-1.0, -0.4472135954999579, 0.4472135954999579, 1.0], jnp.float32)[node_line]
    profile = 1.0 + slope[None, :, :, None] * node_x[:, None, None, None]
    device = (jnp.arange(NE, dtype=jnp.int32) // E_DEV).astype(jnp.float32)
    devices = NE // E_DEV
    rising = 1.0 + 2.0 * device / max(devices - 1, 1)
    values = jnp.exp(jnp.log(0.3) + base * (jnp.log(5.0) - jnp.log(0.3)))
    return (values * rising[None, None, None, :] * profile).astype(jnp.float32)


def draw_depart_coords(key, part):
    shape_slots = (SEGMENTS, GROUPS, 3, GROUPS, CAP)
    first_u = jax.random.uniform(jax.random.fold_in(key, 21), shape_slots, jnp.float32)
    second_u = jax.random.uniform(jax.random.fold_in(key, 22), shape_slots, jnp.float32)
    lean = jax.random.uniform(jax.random.fold_in(key, 23), (SEGMENTS, GROUPS, 1, 1, 1), jnp.float32, 0.1, 0.6)
    first = lean + (1.0 - lean) * (2.0 * first_u - 1.0)
    second = 2.0 * second_u - 1.0
    first = jnp.clip(first, -1.0, 1.0)
    return jnp.stack([first, second], 2).astype(jnp.float32)


def set_ends(values, key, smallest, top_value):
    index_at = [jax.random.randint(jax.random.fold_in(key, axis), (), 0, length) for axis, length in enumerate(values.shape)]
    longest = values.shape.index(max(values.shape))
    next_to = index_at[:longest] + [(index_at[longest] + 1) % values.shape[longest]] + index_at[longest + 1:]
    return values.at[tuple(index_at)].set(smallest).at[tuple(next_to)].set(top_value)


def length_profile(count, total, most, skew):
    portions = [(1 << 20) // math.isqrt(grade ** skew) + 1 for grade in range(2, count + 1)]
    rest, holding = total - most - (count - 1), [1] * (count - 1)
    while rest > 0:
        candidates = [i for i in range(count - 1) if holding[i] < most]
        whole, budget = sum([portions[i] for i in candidates]), rest
        for i in candidates:
            more = min(most - holding[i], max(1, budget * portions[i] // whole), rest)
            holding[i] = holding[i] + more
            rest = rest - more
    return np.array([most] + holding)


def uneven(rng, amount, total, limit, skew):
    if amount == 2:
        one = jax.random.randint(rng, (), max(1, total - limit), min(limit, total - 1) + 1)
        return jnp.stack([one, total - one])
    lengths = jnp.asarray(length_profile(amount, total, limit, skew), jnp.int32)
    twos = (amount - 1) // 2
    giver, taker = lengths[1:1 + 2 * twos:2], lengths[2:2 + 2 * twos:2]
    room = jnp.minimum(giver - 1, limit - taker)
    moved = jax.random.randint(jax.random.fold_in(rng, 1), (twos,), 0, 1 << 20) % (room + 1)
    lengths = lengths.at[1:1 + 2 * twos:2].set(giver - moved).at[2:2 + 2 * twos:2].set(taker + moved)
    return lengths[jax.random.permutation(jax.random.fold_in(rng, 2), amount)]


def setup_inputs(seed: int = 0) -> dict:
    keys = jax.random.split(jax.random.key(seed), 6)
    tracers = draw_tracers(jax.random.fold_in(keys[5], 71), 0)
    send_counts = jax.vmap(lambda own: uneven(own, PEERS, NODES * E_DEV, CAP, 2))(jax.random.split(keys[1], SEGMENTS * GROUPS)).reshape((SEGMENTS, GROUPS, PEERS)).astype(jnp.int32)
    point_order = jax.vmap(lambda own: jax.random.permutation(own, NODES * E_DEV))(jax.random.split(keys[2], SEGMENTS * GROUPS)).reshape((SEGMENTS, GROUPS, POINTS)).astype(jnp.int32)
    depart_elem = set_ends(jax.random.randint(keys[3], (SEGMENTS, GROUPS, 3, GROUPS, CAP), 0, E_DEV), jax.random.fold_in(keys[3], 1), 0, E_DEV - 1).astype(jnp.int32)
    depart_coords = draw_depart_coords(jax.random.fold_in(keys[5], 71), 0)
    return dict(tracers=tracers, send_counts=send_counts, point_order=point_order, depart_elem=depart_elem, depart_coords=depart_coords)


NODE_COORD = (-1.0, -0.4472135954999579, 0.4472135954999579, 1.0)
NODE_WEIGHT = (1.0 / 6.0, 5.0 / 6.0, 5.0 / 6.0, 1.0 / 6.0)


def lagrange(coordinate):
    basis_values = []
    for row_node in range(4):
        weighted = jnp.ones_like(coordinate)
        for other_node in range(4):
            if other_node != row_node:
                weighted = weighted * ((coordinate - NODE_COORD[other_node]) / (NODE_COORD[row_node] - NODE_COORD[other_node]))
        basis_values.append(weighted)
    return basis_values


def interpolate(tracer_field, source_row, first, second):
    along_first = lagrange(first)
    along_second = lagrange(second)
    running_sum = None
    for row_node in range(4):
        for column_node in range(4):
            node_plane = jnp.take(tracer_field[4 * row_node + column_node], source_row, axis=1)
            weighted = (along_first[row_node] * along_second[column_node]) * node_plane
            if running_sum is None:
                running_sum, lower_bound, upper_bound = weighted, node_plane, node_plane
            else:
                running_sum = running_sum + weighted
                lower_bound = jnp.minimum(lower_bound, node_plane)
                upper_bound = jnp.maximum(upper_bound, node_plane)
    return jnp.clip(running_sum, lower_bound, upper_bound)


def quad_table():
    return jnp.array([NODE_WEIGHT[a] * NODE_WEIGHT[b] for a in range(4) for b in range(4)], jnp.float32)


def reference(tracers, send_counts, point_order, depart_elem, depart_coords):
    channels = LEVELS * TRACERS
    devices = SEGMENTS * GROUPS
    tracer_field = tracers.reshape(NODES, channels, NE)
    counts_all = send_counts.reshape(devices, PEERS)
    order_all = point_order.reshape(devices, POINTS)
    elem_all = depart_elem.reshape(devices, PEERS, CAP)
    coord_all = depart_coords.reshape(devices, 2, PEERS * CAP)
    slot_index = jnp.arange(CAP, dtype=jnp.int32)
    peer_index = jnp.arange(PEERS, dtype=jnp.int32)
    sfc_side = peer_index // GROUPS
    target = peer_index % GROUPS

    def one_device(device):
        segment = device // GROUPS
        owner_device = ((segment + sfc_side - 1) % SEGMENTS) * GROUPS + target
        counts = counts_all[device]
        offsets = jnp.cumsum(counts) - counts
        source_row = (owner_device[:, None] * E_DEV + elem_all[device]).reshape(-1).astype(jnp.int32)
        coords = coord_all[device]
        values = interpolate(tracer_field, source_row, coords[0], coords[1])
        in_use = slot_index[None, :] < counts[:, None]
        position = jnp.minimum(offsets[:, None] + slot_index[None, :], POINTS - 1).astype(jnp.int32)
        target_point = jnp.where(in_use, order_all[device][position], POINTS).reshape(-1).astype(jnp.int32)
        return jnp.zeros((channels, POINTS), jnp.float32).at[:, target_point].set(values, mode="drop")

    limited = lax.map(one_device, jnp.arange(devices, dtype=jnp.int32))
    limited = limited.reshape(devices, channels, NODES, E_DEV).transpose(2, 1, 0, 3).reshape(NODES, channels, NE)
    quadrature = quad_table()
    old_mass = jnp.sum(jnp.sum(tracer_field, axis=2) * quadrature[:, None], axis=0)
    new_mass = jnp.sum(jnp.sum(limited, axis=2) * quadrature[:, None], axis=0)
    corrected = limited * (old_mass / new_mass)[None, :, None]
    return corrected.reshape(NODES, LEVELS, TRACERS, NE)
```

```python
import jax
import jax.numpy as jnp
from jax import lax
from jax.experimental import pallas as pl
from jax.experimental.pallas import tpu as pltpu
from jax.sharding import PartitionSpec as P

NODE_COORD = (-1.0, -0.4472135954999579, 0.4472135954999579, 1.0)
SIDES = 3
MESH = pl.DeviceIdType.MESH


def lagrange(x):
    values = []
    for i in range(4):
        value = None
        for m in range(4):
            if m != i:
                term = (x - NODE_COORD[m]) * (1.0 / (NODE_COORD[i] - NODE_COORD[m]))
                value = term if value is None else value * term
        values.append(value)
    return values


def line_weight(line):
    return jnp.where((line == 0) | (line == 3), 1.0 / 6.0, 5.0 / 6.0).astype(jnp.float32)


def split_bf16(x):
    high = x.astype(jnp.bfloat16)
    return high, (x - high.astype(jnp.float32)).astype(jnp.bfloat16)


def diagonal(n, start):
    return lax.broadcasted_iota(jnp.int32, (n, 128), 0) + start == lax.broadcasted_iota(
        jnp.int32, (n, 128), 1
    )


def as_row(column, start):
    return jnp.sum(jnp.where(diagonal(column.shape[0], start), column, 0.0), axis=0, keepdims=True)


def as_column(row, n, start):
    return jnp.sum(jnp.where(diagonal(n, start), row, 0.0), axis=1, keepdims=True)


def prep_kernel(elements, counts_ref, order_ref, elem_ref, coord_ref, request_ref, point_ref, order_pad):
    peers, capacity = elem_ref.shape
    rows = order_ref.shape[0]
    order_pad[0:rows, :] = order_ref[...]
    order_pad[rows:, :] = jnp.zeros((order_pad.shape[0] - rows, 128), jnp.int32)
    lane = lax.broadcasted_iota(jnp.int32, (8, 128), 1)
    slot = lane + 128 * lax.broadcasted_iota(jnp.int32, (8, 128), 0)
    offset = jnp.int32(0)
    for k in range(peers):
        count = counts_ref[0, k]
        row, shift = offset // 128, offset % 128
        window = order_pad[pl.ds(row, 8), :]
        window = pltpu.roll(window, (128 - shift) % 128, 1)
        following = pltpu.roll(window, 7, 0)
        window = jnp.where(lane < 128 - shift, window, following)
        window = jnp.where(slot < count, window, -1)
        for part in range(capacity // 128):
            point_ref[k : k + 1, part * 128 : part * 128 + 128] = window[part : part + 1, :]
        offset = offset + count
    point = point_ref[...]
    node = jnp.floor((point.astype(jnp.float32) + 0.5) * (1.0 / elements)).astype(jnp.int32)
    share = jnp.where(point >= 0, line_weight(node // 4) * line_weight(node % 4), 0.0)
    element = elem_ref[...].astype(jnp.float32)
    for k in range(peers):
        request_ref[k, 0:1, :] = element[k : k + 1, :]
        request_ref[k, 1:2, :] = coord_ref[k : k + 1, :]
        request_ref[k, 2:3, :] = coord_ref[peers + k : peers + k + 1, :]
        request_ref[k, 3:4, :] = share[k : k + 1, :]


def split_field(field_ref, high_ref, low_ref, channels):
    nodes = field_ref.shape[0] // channels
    elements = field_ref.shape[1]
    rows, width = high_ref.shape
    high_ref[:, 128:] = jnp.zeros((rows, width - 128), jnp.bfloat16)
    low_ref[:, 128:] = jnp.zeros((rows, width - 128), jnp.bfloat16)
    old = least = most = None
    for n in range(nodes):
        plane = field_ref[n * channels : (n + 1) * channels, :]
        weight = (5.0 if n // 4 in (1, 2) else 1.0) * (5.0 if n % 4 in (1, 2) else 1.0) / 36.0
        old = plane * weight if old is None else old + plane * weight
        least = plane if least is None else jnp.minimum(least, plane)
        most = plane if most is None else jnp.maximum(most, plane)
        high, low = split_bf16(plane)
        high_ref[n * channels : (n + 1) * channels, 0:elements] = high
        low_ref[n * channels : (n + 1) * channels, 0:elements] = low
    for n, plane in ((nodes, least), (nodes + 1, most)):
        high, low = split_bf16(plane)
        high_ref[n * channels : (n + 1) * channels, 0:elements] = high
        low_ref[n * channels : (n + 1) * channels, 0:elements] = low
    return jnp.sum(old, axis=1, keepdims=True)


def interpolate(requests, blocks, value_ref, high_ref, low_ref, gathered_ref):
    channels, capacity = value_ref.shape[1:]
    width = high_ref.shape[1]
    nodes = high_ref.shape[0] // channels - 2
    element = jnp.concatenate([requests[b, 0:1, :] for b in blocks], 1).astype(jnp.int32)
    source = lax.broadcasted_iota(jnp.int32, (width, element.shape[1]), 0)
    chosen = jnp.where(source == element, 1.0, 0.0).astype(jnp.bfloat16)
    gathered_ref[...] = jnp.dot(
        high_ref[...], chosen, preferred_element_type=jnp.float32
    ) + jnp.dot(low_ref[...], chosen, preferred_element_type=jnp.float32)
    mass = None
    for i, b in enumerate(blocks):
        cols = slice(i * capacity, (i + 1) * capacity)
        first = lagrange(requests[b, 1:2, :])
        second = lagrange(requests[b, 2:3, :])
        total = None
        for n in range(nodes):
            term = (first[n // 4] * second[n % 4]) * gathered_ref[n * channels : (n + 1) * channels, cols]
            total = term if total is None else total + term
        total = jnp.maximum(total, gathered_ref[nodes * channels : (nodes + 1) * channels, cols])
        total = jnp.minimum(total, gathered_ref[(nodes + 1) * channels : (nodes + 2) * channels, cols])
        value_ref[b] = total
        part = total * requests[b, 3:4, :]
        mass = part if mass is None else mass + part
    return mass


def scatter(point_ref, blocks, returned, total_ref, masked_ref, elements):
    channels, capacity = returned.shape[1:]
    nodes = total_ref.shape[0] // channels
    width = total_ref.shape[1]
    point = jnp.concatenate([point_ref[pl.ds(b, 1), :] for b in blocks], 1)
    node = jnp.floor((point.astype(jnp.float32) + 0.5) * (1.0 / elements)).astype(jnp.int32)
    element = jnp.where(point >= 0, point - node * elements, -1)
    place = lax.broadcasted_iota(jnp.int32, (width, element.shape[1]), 0)
    spread = jnp.where(place == element, 1.0, 0.0).astype(jnp.bfloat16)
    value = jnp.concatenate([returned[b] for b in blocks], 1)
    high, low = split_bf16(value)
    for n in range(nodes):
        mask = jnp.where(node == n, 1.0, 0.0).astype(jnp.bfloat16)
        masked_ref[0, n * channels : (n + 1) * channels, :] = high * mask
        masked_ref[1, n * channels : (n + 1) * channels, :] = low * mask
    dims = (((1,), (1,)), ((), ()))
    total_ref[...] += lax.dot_general(
        masked_ref[0], spread, dims, preferred_element_type=jnp.float32
    ) + lax.dot_general(masked_ref[1], spread, dims, preferred_element_type=jnp.float32)


def step_kernel(
    sizes, request_ref, point_ref, field_ref, out_ref,
    asked, values, returned, high_ref, low_ref, gathered_ref, total_ref, masked_ref,
    parts, group_mass, line_mass, ring_mass,
    ask_sent, ask_got, back_sent, back_got, mass_sent, mass_got, known,
):
    lines, ring, groups = sizes
    peers, channels, capacity = values.shape
    elements = field_ref.shape[1]
    nodes = out_ref.shape[0] // channels
    sfc, grp = lax.axis_index("sfc"), lax.axis_index("grp")
    segments = lines * ring
    line, place = sfc // ring, sfc % ring

    def at(segment, group):
        return {"sfc": segment, "grp": group}

    def side(u):
        return (2 * (u // groups)) % SIDES

    def owner(u):
        return (sfc + side(u) - 1 + segments) % segments, (grp + 1 + u) % groups

    def asker(u):
        return (sfc - side(u) + 1 + segments) % segments, (grp - 1 - u + 4 * groups) % groups

    def on_line(i):
        return at(((line + i) % lines) * ring + place, grp)

    def on_ring(i):
        return at(line * ring + (place + i + ring) % ring, grp)

    def ask(u):
        segment, group = owner(u)
        return pltpu.make_async_remote_copy(
            request_ref.at[side(u) * groups + group],
            asked.at[side(u) * groups + grp],
            ask_sent.at[u], ask_got.at[u],
            device_id=at(segment, group), device_id_type=MESH,
        )

    def answer(u):
        segment, group = asker(u)
        return pltpu.make_async_remote_copy(
            values.at[side(u) * groups + group],
            returned.at[side(u) * groups + grp],
            back_sent.at[u], back_got.at[u],
            device_id=at(segment, group), device_id_type=MESH,
        )

    def mass_copy(stage, slots, mine, index, device):
        return pltpu.make_async_remote_copy(
            parts.at[stage], slots.at[mine],
            mass_sent.at[index], mass_got.at[index],
            device_id=device, device_id_type=MESH,
        )

    def group_copy(i):
        return mass_copy(0, group_mass, grp, i, at(sfc, (grp + i) % groups))

    def line_copy(i):
        return mass_copy(1, line_mass, line, groups + i, on_line(i))

    def ring_copy(i):
        return mass_copy(2, ring_mass, place, groups + lines + i, on_ring(i))

    def each(count, act, start=0):
        def body(i, carry):
            act(i)
            return carry
        lax.fori_loop(start, count, body, 0)

    def greet(device):
        pl.semaphore_signal(pltpu.get_barrier_semaphore(), inc=1, device_id=device, device_id_type=MESH)

    others = peers - 1
    each(others, lambda u: greet(at(*owner(u))))
    for i in range(1, lines):
        greet(on_line(i))
    for i in (1, -1):
        greet(on_ring(i))

    old = split_field(field_ref, high_ref, low_ref, channels)
    total_ref[...] = jnp.zeros_like(total_ref)
    asked[groups + grp] = request_ref[groups + grp]

    pl.semaphore_wait(pltpu.get_barrier_semaphore(), others + lines - 1 + 2)
    each(others, lambda u: ask(u).start())

    def tell(step):
        for i in (1 << step, -(1 << step)):
            pl.semaphore_signal(known.at[step], inc=1, device_id=on_ring(i), device_id_type=MESH)

    def hear(step):
        pl.semaphore_wait(known.at[step], 2)

    steps = 0
    while (2 << steps) < ring:
        steps += 1
    tell(0)
    for step in range(1, steps - 1):
        hear(step - 1)
        tell(step)

    PAIR = 2

    def work(j, mass):
        @pl.when(j > 0)
        def _():
            for i in range(PAIR):
                answer(PAIR * (j - 1) + i).start()

        for i in range(PAIR):
            @pl.when(PAIR * j + i < others)
            def _():
                ask(PAIR * j + i).wait_recv()

        blocks = [side(PAIR * j + i) * groups + asker(PAIR * j + i)[1] for i in range(PAIR)]
        return mass + interpolate(asked, blocks, values, high_ref, low_ref, gathered_ref)

    rounds = peers // PAIR
    new = jnp.zeros((channels, capacity), jnp.float32)
    new = lax.fori_loop(0, rounds // 2, work, new)
    hear(steps - 2)
    tell(steps - 1)
    new = lax.fori_loop(rounds // 2, rounds, work, new)
    new = jnp.sum(new, axis=1, keepdims=True)
    parts[0] = as_row(old, 0) + as_row(new, channels)
    returned[groups + grp] = values[groups + grp]
    for u in range(PAIR * (rounds - 1), others):
        answer(u).start()
    group_mass[grp] = parts[0]
    each(groups, lambda i: group_copy(i).start(), 1)

    def put(j, carry):
        for i in range(PAIR):
            @pl.when(PAIR * j + i < others)
            def _():
                answer(PAIR * j + i).wait_recv()

        blocks = [side(PAIR * j + i) * groups + owner(PAIR * j + i)[1] for i in range(PAIR)]
        scatter(point_ref, blocks, returned, total_ref, masked_ref, elements)
        return carry

    third = rounds // 4
    lax.fori_loop(0, third, put, 0)
    each(groups, lambda i: group_copy(i).wait_recv(), 1)
    parts[1] = jnp.sum(group_mass[...], axis=0)
    line_mass[line] = parts[1]
    each(others, lambda u: ask(u).wait_send())
    each(lines, lambda i: line_copy(i).start(), 1)
    lax.fori_loop(third, 2 * third, put, 0)
    each(lines, lambda i: line_copy(i).wait_recv(), 1)
    parts[2] = jnp.sum(line_mass[...], axis=0)
    ring_mass[place] = parts[2]
    hear(steps - 1)
    each(ring, lambda i: ring_copy(i).start(), 1)
    lax.fori_loop(2 * third, rounds, put, 0)
    each(ring, lambda i: ring_copy(i).wait_recv(), 1)
    masses = jnp.sum(ring_mass[...], axis=0)
    factor = as_column(masses, channels, 0) / as_column(masses, channels, channels)
    for n in range(nodes):
        rows = slice(n * channels, (n + 1) * channels)
        out_ref[rows, :] = total_ref[rows, 0:elements] * factor
    each(others, lambda u: answer(u).wait_send())
    each(groups, lambda i: group_copy(i).wait_send(), 1)
    each(lines, lambda i: line_copy(i).wait_send(), 1)
    each(ring, lambda i: ring_copy(i).wait_send(), 1)


def in_vmem(count):
    return [pl.BlockSpec(memory_space=pltpu.VMEM)] * count


def prep(counts, order, elem, coords, elements):
    peers, capacity = elem.shape
    rows = order.shape[0]
    return pl.pallas_call(
        lambda *refs: prep_kernel(elements, *refs),
        out_shape=(
            jax.ShapeDtypeStruct((peers, 4, capacity), jnp.float32),
            jax.ShapeDtypeStruct((peers, capacity), jnp.int32),
        ),
        in_specs=[pl.BlockSpec(memory_space=pltpu.SMEM)] + in_vmem(3),
        out_specs=tuple(in_vmem(2)),
        scratch_shapes=[pltpu.VMEM((rows + 8, 128), jnp.int32)],
        name="prep",
    )(counts, order, elem, coords)


def step(request, point, field, channels, sizes):
    peers, _, capacity = request.shape
    rows, elements = field.shape
    width = -(-elements // 256) * 256
    lines, ring, groups = sizes
    messages = groups + lines + ring
    blocks = pltpu.VMEM((peers, channels, capacity), jnp.float32)
    table = pltpu.VMEM((rows + 2 * channels, width), jnp.bfloat16)
    dma = pltpu.SemaphoreType.DMA
    return pl.pallas_call(
        lambda *refs: step_kernel(sizes, *refs),
        out_shape=jax.ShapeDtypeStruct((rows, elements), jnp.float32),
        in_specs=in_vmem(3),
        out_specs=pl.BlockSpec(memory_space=pltpu.VMEM),
        scratch_shapes=[
            pltpu.VMEM((peers, 4, capacity), jnp.float32),
            blocks,
            blocks,
            table,
            table,
            pltpu.VMEM((rows + 2 * channels, 2 * capacity), jnp.float32),
            pltpu.VMEM((rows, width), jnp.float32),
            pltpu.VMEM((2, rows, 2 * capacity), jnp.bfloat16),
            pltpu.VMEM((3, 1, 128), jnp.float32),
            pltpu.VMEM((groups, 1, 128), jnp.float32),
            pltpu.VMEM((lines, 1, 128), jnp.float32),
            pltpu.VMEM((ring, 1, 128), jnp.float32),
            dma((peers,)), dma((peers,)), dma((peers,)), dma((peers,)),
            dma((messages,)), dma((messages,)),
            pltpu.SemaphoreType.REGULAR((8,)),
        ],
        compiler_params=pltpu.CompilerParams(collective_id=0, has_side_effects=True),
        name="step",
    )(request, point, field)


def local(lines, tracers, send_counts, point_order, depart_elem, depart_coords):
    nodes, levels, species, elements = tracers.shape
    channels = levels * species
    groups, capacity = depart_elem.shape[-2:]
    peers = SIDES * groups
    field = tracers.reshape(nodes * channels, elements)
    request, point = prep(
        send_counts.reshape(1, peers),
        point_order.reshape(-1, 128),
        depart_elem.reshape(peers, capacity),
        depart_coords.reshape(2 * peers, capacity),
        elements,
    )
    sizes = (lines, lax.axis_size("sfc") // lines, groups)
    out = step(request, point, field, channels, sizes)
    return out.reshape(nodes, levels, species, elements)


def solution(mesh, lines=4):
    both = ("sfc", "grp")
    return jax.shard_map(
        lambda *args: local(lines, *args),
        mesh=mesh,
        in_specs=(
            P(None, None, None, both),
            P("sfc", "grp", None),
            P("sfc", "grp", None),
            P("sfc", "grp", None, None, None),
            P("sfc", "grp", None, None, None, None),
        ),
        out_specs=P(None, None, None, both),
        check_vma=False,
    )
```

```python
import jax
import jax.numpy as jnp
from jax import lax
from jax.experimental import pallas as pl
from jax.experimental.pallas import tpu as pltpu
from jax.sharding import PartitionSpec as P

NODE_COORD = (-1.0, -0.4472135954999579, 0.4472135954999579, 1.0)
SIDES = 3
BATCH = 4
MESH = pl.DeviceIdType.MESH


def lagrange(x):
    values = []
    for i in range(4):
        value = None
        for m in range(4):
            if m != i:
                term = (x - NODE_COORD[m]) * (1.0 / (NODE_COORD[i] - NODE_COORD[m]))
                value = term if value is None else value * term
        values.append(value)
    return values


def line_weight(line):
    return jnp.where((line == 0) | (line == 3), 1.0 / 6.0, 5.0 / 6.0).astype(jnp.float32)


def split_bf16(x):
    high = x.astype(jnp.bfloat16)
    return high, (x - high.astype(jnp.float32)).astype(jnp.bfloat16)


def diagonal(n, start):
    return lax.broadcasted_iota(jnp.int32, (n, 128), 0) + start == lax.broadcasted_iota(
        jnp.int32, (n, 128), 1
    )


def as_row(column, start):
    return jnp.sum(jnp.where(diagonal(column.shape[0], start), column, 0.0), axis=0, keepdims=True)


def as_column(row, n, start):
    return jnp.sum(jnp.where(diagonal(n, start), row, 0.0), axis=1, keepdims=True)


def prepare(elements, counts_ref, order_pad, elem_ref, coord_ref, request_ref, point_ref):
    peers, capacity = elem_ref.shape
    lane = lax.broadcasted_iota(jnp.int32, (8, 128), 1)
    slot = lane + 128 * lax.broadcasted_iota(jnp.int32, (8, 128), 0)
    offset = jnp.int32(0)
    counts, shifts, windows = [], [], []
    for k in range(peers):
        counts.append(counts_ref[0, k])
        shifts.append(jnp.full((8, 128), offset & 127))
        windows.append(order_pad[pl.ds(offset >> 7, 8), :])
        offset = offset + counts[k]
    for bit in range(7):
        step = 1 << bit
        windows = [
            jnp.where((shift & step) != 0, pltpu.roll(window, 128 - step, 1), window)
            for shift, window in zip(shifts, windows)
        ]
    for k in range(peers):
        window = jnp.where(lane < 128 - shifts[k], windows[k], pltpu.roll(windows[k], 7, 0))
        window = jnp.where(slot < counts[k], window, -1)
        for part in range(capacity // 128):
            point_ref[k : k + 1, part * 128 : part * 128 + 128] = window[part : part + 1, :]
    point = point_ref[...]
    node = jnp.floor((point.astype(jnp.float32) + 0.5) * (1.0 / elements)).astype(jnp.int32)
    share = jnp.where(point >= 0, line_weight(node >> 2) * line_weight(node & 3), 0.0)
    element = elem_ref[...].astype(jnp.float32)
    for k in range(peers):
        request_ref[k, 0:1, :] = element[k : k + 1, :]
        request_ref[k, 1:2, :] = coord_ref[k : k + 1, :]
        request_ref[k, 2:3, :] = coord_ref[peers + k : peers + k + 1, :]
        request_ref[k, 3:4, :] = share[k : k + 1, :]


def split_field(field_ref, high_ref, low_ref, channels):
    nodes = field_ref.shape[0] // channels
    elements = field_ref.shape[1]
    rows, width = high_ref.shape
    high_ref[:, 128:] = jnp.zeros((rows, width - 128), jnp.bfloat16)
    low_ref[:, 128:] = jnp.zeros((rows, width - 128), jnp.bfloat16)
    old = least = most = None
    for n in range(nodes):
        plane = field_ref[n * channels : (n + 1) * channels, :]
        weight = (5.0 if n // 4 in (1, 2) else 1.0) * (5.0 if n % 4 in (1, 2) else 1.0) / 36.0
        old = plane * weight if old is None else old + plane * weight
        least = plane if least is None else jnp.minimum(least, plane)
        most = plane if most is None else jnp.maximum(most, plane)
        high, low = split_bf16(plane)
        high_ref[n * channels : (n + 1) * channels, 0:elements] = high
        low_ref[n * channels : (n + 1) * channels, 0:elements] = low
    for n, plane in ((nodes, least), (nodes + 1, most)):
        high, low = split_bf16(plane)
        high_ref[n * channels : (n + 1) * channels, 0:elements] = high
        low_ref[n * channels : (n + 1) * channels, 0:elements] = low
    return jnp.sum(old, axis=1, keepdims=True)


def interpolate(requests, blocks, value_ref, high_ref, low_ref, gathered_ref):
    channels, capacity = value_ref.shape[1:]
    width = high_ref.shape[1]
    nodes = high_ref.shape[0] // channels - 2
    element = jnp.concatenate([requests[b, 0:1, :] for b in blocks], 1).astype(jnp.int32)
    source = lax.broadcasted_iota(jnp.int32, (width, element.shape[1]), 0)
    chosen = jnp.where(source == element, 1.0, 0.0).astype(jnp.bfloat16)
    gathered_ref[...] = jnp.dot(
        high_ref[...], chosen, preferred_element_type=jnp.float32
    ) + jnp.dot(low_ref[...], chosen, preferred_element_type=jnp.float32)
    mass = None
    for i, b in enumerate(blocks):
        cols = slice(i * capacity, (i + 1) * capacity)
        first = lagrange(requests[b, 1:2, :])
        second = lagrange(requests[b, 2:3, :])
        total = None
        for n in range(nodes):
            term = (first[n // 4] * second[n % 4]) * gathered_ref[n * channels : (n + 1) * channels, cols]
            total = term if total is None else total + term
        total = jnp.maximum(total, gathered_ref[nodes * channels : (nodes + 1) * channels, cols])
        total = jnp.minimum(total, gathered_ref[(nodes + 1) * channels : (nodes + 2) * channels, cols])
        value_ref[b] = total
        part = total * requests[b, 3:4, :]
        mass = part if mass is None else mass + part
    return mass


def scatter(point_ref, blocks, returned, total_ref, masked_ref, elements):
    channels, capacity = returned.shape[1:]
    nodes = total_ref.shape[0] // channels
    width = total_ref.shape[1]
    point = jnp.concatenate([point_ref[pl.ds(b, 1), :] for b in blocks], 1)
    node = jnp.floor((point.astype(jnp.float32) + 0.5) * (1.0 / elements)).astype(jnp.int32)
    element = jnp.where(point >= 0, point - node * elements, -1)
    place = lax.broadcasted_iota(jnp.int32, (width, element.shape[1]), 0)
    spread = jnp.where(place == element, 1.0, 0.0).astype(jnp.bfloat16)
    value = jnp.concatenate([returned[b] for b in blocks], 1)
    high, low = split_bf16(value)
    for n in range(nodes):
        mask = jnp.where(node == n, 1.0, 0.0).astype(jnp.bfloat16)
        masked_ref[0, n * channels : (n + 1) * channels, :] = high * mask
        masked_ref[1, n * channels : (n + 1) * channels, :] = low * mask
    dims = (((1,), (1,)), ((), ()))
    total_ref[...] += lax.dot_general(
        masked_ref[0], spread, dims, preferred_element_type=jnp.float32
    ) + lax.dot_general(masked_ref[1], spread, dims, preferred_element_type=jnp.float32)


def step_kernel(
    sizes, counts_hbm, order_hbm, elem_hbm, coord_hbm, field_hbm, total_ref, factor_ref,
    counts_ref, order_pad, elem_ref, coord_ref, field_ref, request_ref, point_ref,
    asked, values, returned, high_ref, low_ref, gathered_ref, masked_ref,
    parts, plane_mass, ring_mass,
    loaded, ask_sent, ask_got, back_sent, back_got, plane_sent, plane_got, ring_sent, ring_got, known,
):
    lines, ring, groups = sizes
    peers, channels, capacity = values.shape
    elements = field_ref.shape[1]
    sfc, grp = lax.axis_index("sfc"), lax.axis_index("grp")
    segments = lines * ring
    line, place = sfc // ring, sfc % ring
    others = peers - 1

    loads = [
        pltpu.make_async_copy(counts_hbm, counts_ref, loaded.at[0]),
        pltpu.make_async_copy(order_hbm, order_pad.at[pl.ds(0, order_hbm.shape[0])], loaded.at[1]),
        pltpu.make_async_copy(elem_hbm, elem_ref, loaded.at[2]),
        pltpu.make_async_copy(coord_hbm, coord_ref, loaded.at[3]),
        pltpu.make_async_copy(field_hbm, field_ref, loaded.at[4]),
    ]
    for load in loads:
        load.start()

    def at(segment, group):
        return {"sfc": segment, "grp": group}

    near = [(sfc + segments + side - 1) % segments for side in range(SIDES)]
    ahead = [(grp + i) % groups for i in range(groups)]
    behind = [(grp + groups - i) % groups for i in range(groups)]

    def side(u):
        return (2 * (u // groups)) % SIDES

    def owner(u):
        if isinstance(u, int):
            return near[side(u)], ahead[(1 + u) % groups]
        return (sfc + side(u) - 1 + segments) % segments, (grp + 1 + u) % groups

    def asker(u):
        if isinstance(u, int):
            return near[SIDES - 1 - side(u)], behind[(1 + u) % groups]
        return (sfc - side(u) + 1 + segments) % segments, (grp - 1 - u + 4 * groups) % groups

    def on_line(i, group):
        return at(((line + i) % lines) * ring + place, group)

    def on_ring(i):
        return at(line * ring + (place + i + ring) % ring, grp)

    def ask(u):
        segment, group = owner(u)
        return pltpu.make_async_remote_copy(
            request_ref.at[side(u) * groups + group],
            asked.at[side(u) * groups + grp],
            ask_sent, ask_got.at[u],
            device_id=at(segment, group), device_id_type=MESH,
        )

    def answer(u):
        segment, group = asker(u)
        return pltpu.make_async_remote_copy(
            values.at[side(u) * groups + group],
            returned.at[side(u) * groups + grp],
            back_sent, back_got.at[u],
            device_id=at(segment, group), device_id_type=MESH,
        )

    def plane_copy(i):
        group = (grp + i) % groups
        return pltpu.make_async_remote_copy(
            parts.at[0], plane_mass.at[line * groups + grp], plane_sent, plane_got,
            device_id=on_line(i // groups, group), device_id_type=MESH,
        )

    def ring_copy(i):
        return pltpu.make_async_remote_copy(
            parts.at[1], ring_mass.at[place], ring_sent, ring_got,
            device_id=on_ring(i), device_id_type=MESH,
        )

    def settle(ref, count, semaphore):
        part = ref.at[pl.ds(0, count)]
        pltpu.make_async_copy(part, part, semaphore).wait()

    barrier = pltpu.get_barrier_semaphore()

    def greet(device):
        pl.semaphore_signal(barrier, inc=1, device_id=device, device_id_type=MESH)

    for u in range(others):
        greet(at(*owner(u)))
    for i in range(1, lines):
        greet(on_line(i, grp))
    for i in (1, -1):
        greet(on_ring(i))

    for load in loads[:4]:
        load.wait()
    prepare(elements, counts_ref, order_pad, elem_ref, coord_ref, request_ref, point_ref)
    asked[groups + grp] = request_ref[groups + grp]

    pl.semaphore_wait(barrier, others + lines - 1 + 2)
    for u in range(others):
        ask(u).start()

    def tell(step):
        for i in (1 << step, -(1 << step)):
            pl.semaphore_signal(known.at[step], inc=1, device_id=on_ring(i), device_id_type=MESH)

    def hear(step):
        pl.semaphore_wait(known.at[step], 2)

    steps = 0
    while (2 << steps) < ring:
        steps += 1
    tell(0)
    loads[4].wait()
    old = split_field(field_ref, high_ref, low_ref, channels)
    for step in range(1, steps - 1):
        hear(step - 1)
        tell(step)
    total_ref[...] = jnp.zeros_like(total_ref)

    plane = lines * groups
    rounds = peers // BATCH
    early = groups
    new = jnp.zeros((channels, capacity), jnp.float32)
    for j in range(rounds):
        batch = range(BATCH * j, BATCH * (j + 1))
        for u in range(BATCH * (j - 1), BATCH * j):
            if 0 <= u < early:
                answer(u).start()
        for u in batch:
            if u < others:
                ask(u).wait_recv()
        blocks = [side(u) * groups + asker(u)[1] for u in batch]
        new = new + interpolate(asked, blocks, values, high_ref, low_ref, gathered_ref)
        if j == rounds // 2:
            hear(steps - 2)
            tell(steps - 1)
    new = jnp.sum(new, axis=1, keepdims=True)
    parts[0] = as_row(old, 0) + as_row(new, channels)
    returned[groups + grp] = values[groups + grp]
    plane_mass[line * groups + grp] = parts[0]
    far = sorted(range(1, plane), key=lambda i: -min(i // groups, lines - i // groups) * groups - min(i % groups, groups - i % groups))
    for i in far:
        plane_copy(i).start()
    for u in range(early, others):
        answer(u).start()
    settle(plane_mass, plane - 1, plane_got)
    parts[1] = jnp.sum(plane_mass[...], axis=0)
    hear(steps - 1)
    ring_mass[place] = parts[1]
    for i in sorted(range(1, ring), key=lambda i: -min(i, ring - i)):
        ring_copy(i).start()

    def put(j, carry):
        for i in range(2):
            @pl.when(2 * j + i < others)
            def _():
                answer(2 * j + i).wait_recv()

        blocks = [side(2 * j + i) * groups + owner(2 * j + i)[1] for i in range(2)]
        scatter(point_ref, blocks, returned, total_ref, masked_ref, elements)
        return carry

    lax.fori_loop(0, peers // 2, put, 0)
    settle(request_ref, others, ask_sent)
    settle(values, others, back_sent)
    settle(plane_mass, plane - 1, plane_sent)
    settle(ring_mass, ring - 1, ring_sent)
    settle(ring_mass, ring - 1, ring_got)
    masses = jnp.sum(ring_mass[...], axis=0)
    factor = as_column(masses, channels, 0) / as_column(masses, channels, channels)
    factor_ref[...] = jnp.broadcast_to(factor, factor_ref.shape)


def step(counts, order, elem, coords, field, channels, sizes):
    peers, capacity = elem.shape
    rows, elements = field.shape
    width = -(-elements // 256) * 256
    lines, ring, groups = sizes
    vmem, dma = pltpu.VMEM, pltpu.SemaphoreType.DMA
    blocks = vmem((peers, channels, capacity), jnp.float32)
    table = vmem((rows + 2 * channels, width), jnp.bfloat16)
    plane = lines * groups
    return pl.pallas_call(
        lambda *refs: step_kernel(sizes, *refs),
        out_shape=(
            jax.ShapeDtypeStruct((rows, width), jnp.float32),
            jax.ShapeDtypeStruct((channels, width), jnp.float32),
        ),
        in_specs=[pl.BlockSpec(memory_space=pltpu.HBM)] * 5,
        out_specs=(pl.BlockSpec(memory_space=pltpu.VMEM),) * 2,
        scratch_shapes=[
            pltpu.SMEM(counts.shape, jnp.int32),
            vmem((order.shape[0] + 8, 128), jnp.int32),
            vmem(elem.shape, jnp.int32),
            vmem(coords.shape, jnp.float32),
            vmem(field.shape, jnp.float32),
            vmem((peers, 4, capacity), jnp.float32),
            vmem((peers, capacity), jnp.int32),
            vmem((peers, 4, capacity), jnp.float32),
            blocks,
            blocks,
            table,
            table,
            vmem((rows + 2 * channels, BATCH * capacity), jnp.float32),
            vmem((2, rows, 2 * capacity), jnp.bfloat16),
            vmem((2, 1, 128), jnp.float32),
            vmem((plane, 1, 128), jnp.float32),
            vmem((ring, 1, 128), jnp.float32),
            dma((5,)),
            dma(()), dma((peers,)), dma(()), dma((peers,)),
            dma(()), dma(()), dma(()), dma(()),
            pltpu.SemaphoreType.REGULAR((8,)),
        ],
        compiler_params=pltpu.CompilerParams(
            collective_id=0, has_side_effects=True, vmem_limit_bytes=24 << 20
        ),
        name="step",
    )(*(pltpu.with_memory_space_constraint(x, pltpu.HBM) for x in (counts, order, elem, coords, field)))


def local(lines, tracers, send_counts, point_order, depart_elem, depart_coords):
    nodes, levels, species, elements = tracers.shape
    channels = levels * species
    groups, capacity = depart_elem.shape[-2:]
    peers = SIDES * groups
    total, factor = step(
        send_counts.reshape(1, peers),
        point_order.reshape(-1, 128),
        depart_elem.reshape(peers, capacity),
        depart_coords.reshape(2 * peers, capacity),
        tracers.reshape(nodes * channels, elements),
        channels,
        (lines, lax.axis_size("sfc") // lines, groups),
    )
    out = total.reshape(nodes, channels, -1)[:, :, :elements] * factor[None, :, :elements]
    return out.reshape(nodes, levels, species, elements)


def solution(mesh, lines=4):
    both = ("sfc", "grp")
    return jax.shard_map(
        lambda *args: local(lines, *args),
        mesh=mesh,
        in_specs=(
            P(None, None, None, both),
            P("sfc", "grp", None),
            P("sfc", "grp", None),
            P("sfc", "grp", None, None, None),
            P("sfc", "grp", None, None, None, None),
        ),
        out_specs=P(None, None, None, both),
        check_vma=False,
    )
```

```python
import jax
import jax.numpy as jnp
from jax import lax
from jax.experimental import pallas as pl
from jax.experimental.pallas import tpu as pltpu
from jax.sharding import PartitionSpec as P

NODE_COORD = (-1.0, -0.4472135954999579, 0.4472135954999579, 1.0)
SIDES = 3
BATCH = 4
MESH = pl.DeviceIdType.MESH


def lagrange(x):
    values = []
    for i in range(4):
        value = None
        for m in range(4):
            if m != i:
                term = (x - NODE_COORD[m]) * (1.0 / (NODE_COORD[i] - NODE_COORD[m]))
                value = term if value is None else value * term
        values.append(value)
    return values


def line_weight(line):
    return jnp.where((line == 0) | (line == 3), 1.0 / 6.0, 5.0 / 6.0).astype(jnp.float32)


def split_bf16(x):
    high = x.astype(jnp.bfloat16)
    return high, (x - high.astype(jnp.float32)).astype(jnp.bfloat16)


def diagonal(n, start):
    return lax.broadcasted_iota(jnp.int32, (n, 128), 0) + start == lax.broadcasted_iota(
        jnp.int32, (n, 128), 1
    )


def as_row(column, start):
    return jnp.sum(jnp.where(diagonal(column.shape[0], start), column, 0.0), axis=0, keepdims=True)


def as_column(row, n, start):
    return jnp.sum(jnp.where(diagonal(n, start), row, 0.0), axis=1, keepdims=True)


def prepare(elements, counts_ref, order_pad, elem_ref, coord_ref, request_ref, point_ref):
    peers, capacity = elem_ref.shape
    lane = lax.broadcasted_iota(jnp.int32, (8, 128), 1)
    slot = lane + 128 * lax.broadcasted_iota(jnp.int32, (8, 128), 0)
    offset = jnp.int32(0)
    counts, shifts, windows = [], [], []
    for k in range(peers):
        counts.append(counts_ref[0, k])
        shifts.append(jnp.full((8, 128), offset & 127))
        windows.append(order_pad[pl.ds(offset >> 7, 8), :])
        offset = offset + counts[k]
    for bit in range(7):
        step = 1 << bit
        windows = [
            jnp.where((shift & step) != 0, pltpu.roll(window, 128 - step, 1), window)
            for shift, window in zip(shifts, windows)
        ]
    for k in range(peers):
        window = jnp.where(lane < 128 - shifts[k], windows[k], pltpu.roll(windows[k], 7, 0))
        window = jnp.where(slot < counts[k], window, -1)
        for part in range(capacity // 128):
            point_ref[k : k + 1, part * 128 : part * 128 + 128] = window[part : part + 1, :]
    point = point_ref[...]
    node = jnp.floor((point.astype(jnp.float32) + 0.5) * (1.0 / elements)).astype(jnp.int32)
    share = jnp.where(point >= 0, line_weight(node >> 2) * line_weight(node & 3), 0.0)
    element = elem_ref[...].astype(jnp.float32)
    for k in range(peers):
        request_ref[k, 0:1, :] = element[k : k + 1, :]
        request_ref[k, 1:2, :] = coord_ref[k : k + 1, :]
        request_ref[k, 2:3, :] = coord_ref[peers + k : peers + k + 1, :]
        request_ref[k, 3:4, :] = share[k : k + 1, :]


def split_field(field_ref, high_ref, low_ref, channels):
    nodes = field_ref.shape[0] // channels
    elements = field_ref.shape[1]
    rows, width = high_ref.shape
    high_ref[:, 128:] = jnp.zeros((rows, width - 128), jnp.bfloat16)
    low_ref[:, 128:] = jnp.zeros((rows, width - 128), jnp.bfloat16)
    old = least = most = None
    for n in range(nodes):
        plane = field_ref[n * channels : (n + 1) * channels, :]
        weight = (5.0 if n // 4 in (1, 2) else 1.0) * (5.0 if n % 4 in (1, 2) else 1.0) / 36.0
        old = plane * weight if old is None else old + plane * weight
        least = plane if least is None else jnp.minimum(least, plane)
        most = plane if most is None else jnp.maximum(most, plane)
        high, low = split_bf16(plane)
        high_ref[n * channels : (n + 1) * channels, 0:elements] = high
        low_ref[n * channels : (n + 1) * channels, 0:elements] = low
    for n, plane in ((nodes, least), (nodes + 1, most)):
        high, low = split_bf16(plane)
        high_ref[n * channels : (n + 1) * channels, 0:elements] = high
        low_ref[n * channels : (n + 1) * channels, 0:elements] = low
    return jnp.sum(old, axis=1, keepdims=True)


def interpolate(requests, blocks, value_ref, high_ref, low_ref, gathered_ref):
    channels, capacity = value_ref.shape[1:]
    width = high_ref.shape[1]
    nodes = high_ref.shape[0] // channels - 2
    element = jnp.concatenate([requests[b, 0:1, :] for b in blocks], 1).astype(jnp.int32)
    source = lax.broadcasted_iota(jnp.int32, (width, element.shape[1]), 0)
    chosen = jnp.where(source == element, 1.0, 0.0).astype(jnp.bfloat16)
    gathered_ref[...] = jnp.dot(
        high_ref[...], chosen, preferred_element_type=jnp.float32
    ) + jnp.dot(low_ref[...], chosen, preferred_element_type=jnp.float32)
    mass = None
    for i, b in enumerate(blocks):
        cols = slice(i * capacity, (i + 1) * capacity)
        first = lagrange(requests[b, 1:2, :])
        second = lagrange(requests[b, 2:3, :])
        total = None
        for n in range(nodes):
            term = (first[n // 4] * second[n % 4]) * gathered_ref[n * channels : (n + 1) * channels, cols]
            total = term if total is None else total + term
        total = jnp.maximum(total, gathered_ref[nodes * channels : (nodes + 1) * channels, cols])
        total = jnp.minimum(total, gathered_ref[(nodes + 1) * channels : (nodes + 2) * channels, cols])
        value_ref[b] = total
        part = total * requests[b, 3:4, :]
        mass = part if mass is None else mass + part
    return mass


def scatter(point_ref, blocks, returned, total_ref, masked_ref, elements):
    channels, capacity = returned.shape[1:]
    nodes = total_ref.shape[0] // channels
    width = total_ref.shape[1]
    point = jnp.concatenate([point_ref[pl.ds(b, 1), :] for b in blocks], 1)
    node = jnp.floor((point.astype(jnp.float32) + 0.5) * (1.0 / elements)).astype(jnp.int32)
    element = jnp.where(point >= 0, point - node * elements, -1)
    place = lax.broadcasted_iota(jnp.int32, (width, element.shape[1]), 0)
    spread = jnp.where(place == element, 1.0, 0.0).astype(jnp.bfloat16)
    value = jnp.concatenate([returned[b] for b in blocks], 1)
    high, low = split_bf16(value)
    for n in range(nodes):
        mask = jnp.where(node == n, 1.0, 0.0).astype(jnp.bfloat16)
        masked_ref[0, n * channels : (n + 1) * channels, :] = high * mask
        masked_ref[1, n * channels : (n + 1) * channels, :] = low * mask
    dims = (((1,), (1,)), ((), ()))
    total_ref[...] += lax.dot_general(
        masked_ref[0], spread, dims, preferred_element_type=jnp.float32
    ) + lax.dot_general(masked_ref[1], spread, dims, preferred_element_type=jnp.float32)


def step_kernel(
    sizes, counts_hbm, order_hbm, elem_hbm, coord_hbm, field_hbm, total_ref, factor_ref,
    counts_ref, order_pad, elem_ref, coord_ref, field_ref, request_ref, point_ref,
    asked, values, returned, high_ref, low_ref, gathered_ref, masked_ref,
    parts, plane_mass, ring_mass,
    loaded, ask_sent, ask_got, back_sent, back_got, plane_sent, plane_got, ring_sent, ring_got, known,
):
    lines, ring, groups = sizes
    peers, channels, capacity = values.shape
    elements = field_ref.shape[1]
    sfc, grp = lax.axis_index("sfc"), lax.axis_index("grp")
    segments = lines * ring
    line, place = sfc // ring, sfc % ring
    others = peers - 1

    loads = [
        pltpu.make_async_copy(counts_hbm, counts_ref, loaded.at[0]),
        pltpu.make_async_copy(order_hbm, order_pad.at[pl.ds(0, order_hbm.shape[0])], loaded.at[1]),
        pltpu.make_async_copy(elem_hbm, elem_ref, loaded.at[2]),
        pltpu.make_async_copy(coord_hbm, coord_ref, loaded.at[3]),
        pltpu.make_async_copy(field_hbm, field_ref, loaded.at[4]),
    ]
    for load in loads:
        load.start()

    def at(segment, group):
        return {"sfc": segment, "grp": group}

    near = [(sfc + segments + side - 1) % segments for side in range(SIDES)]
    ahead = [(grp + i) % groups for i in range(groups)]
    behind = [(grp + groups - i) % groups for i in range(groups)]

    def side(u):
        return (2 * (u // groups)) % SIDES

    def owner(u):
        if isinstance(u, int):
            return near[side(u)], ahead[(1 + u) % groups]
        return (sfc + side(u) - 1 + segments) % segments, (grp + 1 + u) % groups

    def asker(u):
        if isinstance(u, int):
            return near[SIDES - 1 - side(u)], behind[(1 + u) % groups]
        return (sfc - side(u) + 1 + segments) % segments, (grp - 1 - u + 4 * groups) % groups

    def on_line(i, group):
        return at(((line + i) % lines) * ring + place, group)

    def on_ring(i):
        return at(line * ring + (place + i + ring) % ring, grp)

    def ask(u):
        segment, group = owner(u)
        return pltpu.make_async_remote_copy(
            request_ref.at[side(u) * groups + group],
            asked.at[side(u) * groups + grp],
            ask_sent, ask_got.at[u],
            device_id=at(segment, group), device_id_type=MESH,
        )

    def answer(u):
        segment, group = asker(u)
        return pltpu.make_async_remote_copy(
            values.at[side(u) * groups + group],
            returned.at[side(u) * groups + grp],
            back_sent, back_got.at[u],
            device_id=at(segment, group), device_id_type=MESH,
        )

    def plane_copy(i):
        group = (grp + i) % groups
        return pltpu.make_async_remote_copy(
            parts.at[0], plane_mass.at[line * groups + grp], plane_sent, plane_got,
            device_id=on_line(i // groups, group), device_id_type=MESH,
        )

    def ring_copy(i):
        return pltpu.make_async_remote_copy(
            parts.at[1], ring_mass.at[place], ring_sent, ring_got,
            device_id=on_ring(i), device_id_type=MESH,
        )

    def settle(ref, count, semaphore):
        part = ref.at[pl.ds(0, count)]
        pltpu.make_async_copy(part, part, semaphore).wait()

    barrier = pltpu.get_barrier_semaphore()

    def greet(device):
        pl.semaphore_signal(barrier, inc=1, device_id=device, device_id_type=MESH)

    for u in range(others):
        greet(at(*owner(u)))
    for i in range(1, lines):
        greet(on_line(i, grp))
    for i in (1, -1):
        greet(on_ring(i))

    for load in loads[:4]:
        load.wait()
    prepare(elements, counts_ref, order_pad, elem_ref, coord_ref, request_ref, point_ref)
    asked[groups + grp] = request_ref[groups + grp]

    pl.semaphore_wait(barrier, others + lines - 1 + 2)
    for u in range(others):
        ask(u).start()

    def tell(step):
        for i in (1 << step, -(1 << step)):
            pl.semaphore_signal(known.at[step], inc=1, device_id=on_ring(i), device_id_type=MESH)

    def hear(step):
        pl.semaphore_wait(known.at[step], 2)

    steps = 0
    while (2 << steps) < ring:
        steps += 1
    tell(0)
    loads[4].wait()
    old = split_field(field_ref, high_ref, low_ref, channels)
    for step in range(1, steps - 1):
        hear(step - 1)
        tell(step)
    total_ref[...] = jnp.zeros_like(total_ref)

    plane = lines * groups
    rounds = peers // BATCH
    early = groups
    new = jnp.zeros((channels, capacity), jnp.float32)
    for j in range(rounds):
        batch = range(BATCH * j, BATCH * (j + 1))
        for u in range(BATCH * (j - 1), BATCH * j):
            if 0 <= u < early:
                answer(u).start()
        for u in batch:
            if u < others:
                ask(u).wait_recv()
        blocks = [side(u) * groups + asker(u)[1] for u in batch]
        new = new + interpolate(asked, blocks, values, high_ref, low_ref, gathered_ref)
        if j == rounds // 2:
            hear(steps - 2)
            tell(steps - 1)
    new = jnp.sum(new, axis=1, keepdims=True)
    parts[0] = as_row(old, 0) + as_row(new, channels)
    returned[groups + grp] = values[groups + grp]
    plane_mass[line * groups + grp] = parts[0]
    far = sorted(range(1, plane), key=lambda i: -min(i // groups, lines - i // groups) * groups - min(i % groups, groups - i % groups))
    for i in far:
        plane_copy(i).start()
    for u in range(2 * groups, others):
        answer(u).start()
    settle(plane_mass, plane - 1, plane_got)
    parts[1] = jnp.sum(plane_mass[...], axis=0)
    hear(steps - 1)
    ring_mass[place] = parts[1]
    for i in sorted(range(1, ring), key=lambda i: -min(i, ring - i)):
        ring_copy(i).start()
    for u in range(groups, 2 * groups):
        answer(u).start()

    def put(j, carry):
        half = groups // 2
        j = (2 * (j // half)) % SIDES * half + j % half
        for i in range(2):
            @pl.when(2 * j + i < others)
            def _():
                answer(2 * j + i).wait_recv()

        blocks = [side(2 * j + i) * groups + owner(2 * j + i)[1] for i in range(2)]
        scatter(point_ref, blocks, returned, total_ref, masked_ref, elements)
        return carry

    lax.fori_loop(0, peers // 2, put, 0)
    settle(request_ref, others, ask_sent)
    settle(values, others, back_sent)
    settle(plane_mass, plane - 1, plane_sent)
    settle(ring_mass, ring - 1, ring_sent)
    settle(ring_mass, ring - 1, ring_got)
    masses = jnp.sum(ring_mass[...], axis=0)
    factor = as_column(masses, channels, 0) / as_column(masses, channels, channels)
    factor_ref[...] = jnp.broadcast_to(factor, factor_ref.shape)


def step(counts, order, elem, coords, field, channels, sizes):
    peers, capacity = elem.shape
    rows, elements = field.shape
    width = -(-elements // 256) * 256
    lines, ring, groups = sizes
    vmem, dma = pltpu.VMEM, pltpu.SemaphoreType.DMA
    blocks = vmem((peers, channels, capacity), jnp.float32)
    table = vmem((rows + 2 * channels, width), jnp.bfloat16)
    plane = lines * groups
    return pl.pallas_call(
        lambda *refs: step_kernel(sizes, *refs),
        out_shape=(
            jax.ShapeDtypeStruct((rows, width), jnp.float32),
            jax.ShapeDtypeStruct((channels, width), jnp.float32),
        ),
        in_specs=[pl.BlockSpec(memory_space=pltpu.HBM)] * 5,
        out_specs=(pl.BlockSpec(memory_space=pltpu.VMEM),) * 2,
        scratch_shapes=[
            pltpu.SMEM(counts.shape, jnp.int32),
            vmem((order.shape[0] + 8, 128), jnp.int32),
            vmem(elem.shape, jnp.int32),
            vmem(coords.shape, jnp.float32),
            vmem(field.shape, jnp.float32),
            vmem((peers, 4, capacity), jnp.float32),
            vmem((peers, capacity), jnp.int32),
            vmem((peers, 4, capacity), jnp.float32),
            blocks,
            blocks,
            table,
            table,
            vmem((rows + 2 * channels, BATCH * capacity), jnp.float32),
            vmem((2, rows, 2 * capacity), jnp.bfloat16),
            vmem((2, 1, 128), jnp.float32),
            vmem((plane, 1, 128), jnp.float32),
            vmem((ring, 1, 128), jnp.float32),
            dma((5,)),
            dma(()), dma((peers,)), dma(()), dma((peers,)),
            dma(()), dma(()), dma(()), dma(()),
            pltpu.SemaphoreType.REGULAR((8,)),
        ],
        compiler_params=pltpu.CompilerParams(
            collective_id=0, has_side_effects=True, vmem_limit_bytes=24 << 20
        ),
        name="step",
    )(*(pltpu.with_memory_space_constraint(x, pltpu.HBM) for x in (counts, order, elem, coords, field)))


def local(lines, tracers, send_counts, point_order, depart_elem, depart_coords):
    nodes, levels, species, elements = tracers.shape
    channels = levels * species
    groups, capacity = depart_elem.shape[-2:]
    peers = SIDES * groups
    total, factor = step(
        send_counts.reshape(1, peers),
        point_order.reshape(-1, 128),
        depart_elem.reshape(peers, capacity),
        depart_coords.reshape(2 * peers, capacity),
        tracers.reshape(nodes * channels, elements),
        channels,
        (lines, lax.axis_size("sfc") // lines, groups),
    )
    out = total.reshape(nodes, channels, -1)[:, :, :elements] * factor[None, :, :elements]
    return out.reshape(nodes, levels, species, elements)


def solution(mesh, lines=4):
    both = ("sfc", "grp")
    return jax.shard_map(
        lambda *args: local(lines, *args),
        mesh=mesh,
        in_specs=(
            P(None, None, None, both),
            P("sfc", "grp", None),
            P("sfc", "grp", None),
            P("sfc", "grp", None, None, None),
            P("sfc", "grp", None, None, None, None),
        ),
        out_specs=P(None, None, None, both),
        check_vma=False,
    )
```

```python
import jax
import jax.numpy as jnp
from jax import lax
from jax.experimental import pallas as pl
from jax.experimental.pallas import tpu as pltpu
from jax.sharding import PartitionSpec as P

NODE_COORD = (-1.0, -0.4472135954999579, 0.4472135954999579, 1.0)
SIDES = 3
BATCH = 4
MESH = pl.DeviceIdType.MESH


def lagrange(x):
    values = []
    for i in range(4):
        value = None
        for m in range(4):
            if m != i:
                term = (x - NODE_COORD[m]) * (1.0 / (NODE_COORD[i] - NODE_COORD[m]))
                value = term if value is None else value * term
        values.append(value)
    return values


def line_weight(line):
    return jnp.where((line == 0) | (line == 3), 1.0 / 6.0, 5.0 / 6.0).astype(jnp.float32)


def split_bf16(x):
    high = x.astype(jnp.bfloat16)
    return high, (x - high.astype(jnp.float32)).astype(jnp.bfloat16)


def diagonal(n, start):
    return lax.broadcasted_iota(jnp.int32, (n, 128), 0) + start == lax.broadcasted_iota(
        jnp.int32, (n, 128), 1
    )


def as_row(column, start):
    return jnp.sum(jnp.where(diagonal(column.shape[0], start), column, 0.0), axis=0, keepdims=True)


def as_column(row, n, start):
    return jnp.sum(jnp.where(diagonal(n, start), row, 0.0), axis=1, keepdims=True)


def prepare(elements, counts_ref, order_pad, elem_ref, coord_ref, request_ref, point_ref):
    peers, capacity = elem_ref.shape
    lane = lax.broadcasted_iota(jnp.int32, (8, 128), 1)
    slot = lane + 128 * lax.broadcasted_iota(jnp.int32, (8, 128), 0)
    offset = jnp.int32(0)
    counts, shifts, windows = [], [], []
    for k in range(peers):
        counts.append(counts_ref[0, k])
        shifts.append(jnp.full((8, 128), offset & 127))
        windows.append(order_pad[pl.ds(offset >> 7, 8), :])
        offset = offset + counts[k]
    for bit in range(7):
        step = 1 << bit
        windows = [
            jnp.where((shift & step) != 0, pltpu.roll(window, 128 - step, 1), window)
            for shift, window in zip(shifts, windows)
        ]
    for k in range(peers):
        window = jnp.where(lane < 128 - shifts[k], windows[k], pltpu.roll(windows[k], 7, 0))
        window = jnp.where(slot < counts[k], window, -1)
        for part in range(capacity // 128):
            point_ref[k : k + 1, part * 128 : part * 128 + 128] = window[part : part + 1, :]
    point = point_ref[...]
    node = jnp.floor((point.astype(jnp.float32) + 0.5) * (1.0 / elements)).astype(jnp.int32)
    share = jnp.where(point >= 0, line_weight(node >> 2) * line_weight(node & 3), 0.0)
    element = elem_ref[...].astype(jnp.float32)
    for k in range(peers):
        request_ref[k, 0:1, :] = element[k : k + 1, :]
        request_ref[k, 1:2, :] = coord_ref[k : k + 1, :]
        request_ref[k, 2:3, :] = coord_ref[peers + k : peers + k + 1, :]
        request_ref[k, 3:4, :] = share[k : k + 1, :]


def split_field(field_ref, high_ref, low_ref, channels):
    nodes = field_ref.shape[0] // channels
    elements = field_ref.shape[1]
    rows, width = high_ref.shape
    high_ref[:, 128:] = jnp.zeros((rows, width - 128), jnp.bfloat16)
    low_ref[:, 128:] = jnp.zeros((rows, width - 128), jnp.bfloat16)
    old = least = most = None
    for n in range(nodes):
        plane = field_ref[n * channels : (n + 1) * channels, :]
        weight = (5.0 if n // 4 in (1, 2) else 1.0) * (5.0 if n % 4 in (1, 2) else 1.0) / 36.0
        old = plane * weight if old is None else old + plane * weight
        least = plane if least is None else jnp.minimum(least, plane)
        most = plane if most is None else jnp.maximum(most, plane)
        high, low = split_bf16(plane)
        high_ref[n * channels : (n + 1) * channels, 0:elements] = high
        low_ref[n * channels : (n + 1) * channels, 0:elements] = low
    for n, plane in ((nodes, least), (nodes + 1, most)):
        high, low = split_bf16(plane)
        high_ref[n * channels : (n + 1) * channels, 0:elements] = high
        low_ref[n * channels : (n + 1) * channels, 0:elements] = low
    return jnp.sum(old, axis=1, keepdims=True)


def interpolate(requests, blocks, value_ref, high_ref, low_ref, gathered_ref):
    channels, capacity = value_ref.shape[1:]
    width = high_ref.shape[1]
    nodes = high_ref.shape[0] // channels - 2
    element = jnp.concatenate([requests[b, 0:1, :] for b in blocks], 1).astype(jnp.int32)
    source = lax.broadcasted_iota(jnp.int32, (width, element.shape[1]), 0)
    chosen = jnp.where(source == element, 1.0, 0.0).astype(jnp.bfloat16)
    gathered_ref[...] = jnp.dot(
        high_ref[...], chosen, preferred_element_type=jnp.float32
    ) + jnp.dot(low_ref[...], chosen, preferred_element_type=jnp.float32)
    mass = None
    for i, b in enumerate(blocks):
        cols = slice(i * capacity, (i + 1) * capacity)
        first = lagrange(requests[b, 1:2, :])
        second = lagrange(requests[b, 2:3, :])
        total = None
        for n in range(nodes):
            term = (first[n // 4] * second[n % 4]) * gathered_ref[n * channels : (n + 1) * channels, cols]
            total = term if total is None else total + term
        total = jnp.maximum(total, gathered_ref[nodes * channels : (nodes + 1) * channels, cols])
        total = jnp.minimum(total, gathered_ref[(nodes + 1) * channels : (nodes + 2) * channels, cols])
        value_ref[b] = total
        part = total * requests[b, 3:4, :]
        mass = part if mass is None else mass + part
    return mass


def scatter(point_ref, blocks, returned, total_ref, masked_ref, elements):
    channels, capacity = returned.shape[1:]
    nodes = total_ref.shape[0] // channels
    width = total_ref.shape[1]
    point = jnp.concatenate([point_ref[pl.ds(b, 1), :] for b in blocks], 1)
    node = jnp.floor((point.astype(jnp.float32) + 0.5) * (1.0 / elements)).astype(jnp.int32)
    element = jnp.where(point >= 0, point - node * elements, -1)
    place = lax.broadcasted_iota(jnp.int32, (width, element.shape[1]), 0)
    spread = jnp.where(place == element, 1.0, 0.0).astype(jnp.bfloat16)
    value = jnp.concatenate([returned[b] for b in blocks], 1)
    high, low = split_bf16(value)
    for n in range(nodes):
        mask = jnp.where(node == n, 1.0, 0.0).astype(jnp.bfloat16)
        masked_ref[0, n * channels : (n + 1) * channels, :] = high * mask
        masked_ref[1, n * channels : (n + 1) * channels, :] = low * mask
    dims = (((1,), (1,)), ((), ()))
    total_ref[...] += lax.dot_general(
        masked_ref[0], spread, dims, preferred_element_type=jnp.float32
    ) + lax.dot_general(masked_ref[1], spread, dims, preferred_element_type=jnp.float32)


def step_kernel(
    sizes, counts_hbm, order_hbm, elem_hbm, coord_hbm, field_hbm, total_ref, factor_ref,
    counts_ref, order_pad, elem_ref, coord_ref, field_ref, request_ref, point_ref,
    asked, values, returned, high_ref, low_ref, gathered_ref, masked_ref,
    parts, plane_mass, ring_mass,
    loaded, ask_sent, ask_got, back_sent, back_got, plane_sent, plane_got, ring_sent, ring_got, known,
):
    lines, ring, groups = sizes
    peers, channels, capacity = values.shape
    elements = field_ref.shape[1]
    sfc, grp = lax.axis_index("sfc"), lax.axis_index("grp")
    segments = lines * ring
    line, place = sfc // ring, sfc % ring
    others = peers - 1
    itself = groups - 1
    away = [u for u in range(peers) if u != itself]

    loads = [
        pltpu.make_async_copy(counts_hbm, counts_ref, loaded.at[0]),
        pltpu.make_async_copy(order_hbm, order_pad.at[pl.ds(0, order_hbm.shape[0])], loaded.at[1]),
        pltpu.make_async_copy(elem_hbm, elem_ref, loaded.at[2]),
        pltpu.make_async_copy(coord_hbm, coord_ref, loaded.at[3]),
        pltpu.make_async_copy(field_hbm, field_ref, loaded.at[4]),
    ]
    for load in loads:
        load.start()

    def at(segment, group):
        return {"sfc": segment, "grp": group}

    near = [(sfc + segments + side - 1) % segments for side in range(SIDES)]
    ahead = [(grp + i) % groups for i in range(groups)]
    behind = [(grp + groups - i) % groups for i in range(groups)]

    def side(u):
        return (2 * (u // groups) + 1) % SIDES

    def owner(u):
        if isinstance(u, int):
            return near[side(u)], ahead[(1 + u) % groups]
        return (sfc + side(u) - 1 + segments) % segments, (grp + 1 + u) % groups

    def asker(u):
        if isinstance(u, int):
            return near[SIDES - 1 - side(u)], behind[(1 + u) % groups]
        return (sfc - side(u) + 1 + segments) % segments, (grp - 1 - u + 4 * groups) % groups

    def on_line(i, group):
        return at(((line + i) % lines) * ring + place, group)

    def on_ring(i):
        return at(line * ring + (place + i + ring) % ring, grp)

    def ask(u):
        segment, group = owner(u)
        return pltpu.make_async_remote_copy(
            request_ref.at[side(u) * groups + group],
            asked.at[side(u) * groups + grp],
            ask_sent, ask_got.at[u],
            device_id=at(segment, group), device_id_type=MESH,
        )

    def answer(u):
        segment, group = asker(u)
        return pltpu.make_async_remote_copy(
            values.at[side(u) * groups + group],
            returned.at[side(u) * groups + grp],
            back_sent, back_got.at[u],
            device_id=at(segment, group), device_id_type=MESH,
        )

    def plane_copy(i):
        group = (grp + i) % groups
        return pltpu.make_async_remote_copy(
            parts.at[0], plane_mass.at[line * groups + grp], plane_sent, plane_got,
            device_id=on_line(i // groups, group), device_id_type=MESH,
        )

    def ring_copy(i):
        return pltpu.make_async_remote_copy(
            parts.at[1], ring_mass.at[place], ring_sent, ring_got,
            device_id=on_ring(i), device_id_type=MESH,
        )

    def settle(ref, count, semaphore):
        part = ref.at[pl.ds(0, count)]
        pltpu.make_async_copy(part, part, semaphore).wait()

    barrier = pltpu.get_barrier_semaphore()

    def greet(device):
        pl.semaphore_signal(barrier, inc=1, device_id=device, device_id_type=MESH)

    for u in away:
        greet(at(*owner(u)))
    for i in range(1, lines):
        greet(on_line(i, grp))
    for i in (1, -1):
        greet(on_ring(i))

    for load in loads[:4]:
        load.wait()
    prepare(elements, counts_ref, order_pad, elem_ref, coord_ref, request_ref, point_ref)
    asked[groups + grp] = request_ref[groups + grp]

    pl.semaphore_wait(barrier, others + lines - 1 + 2)
    for u in away:
        ask(u).start()

    def tell(step):
        for i in (1 << step, -(1 << step)):
            pl.semaphore_signal(known.at[step], inc=1, device_id=on_ring(i), device_id_type=MESH)

    def hear(step):
        pl.semaphore_wait(known.at[step], 2)

    steps = 0
    while (2 << steps) < ring:
        steps += 1
    tell(0)
    loads[4].wait()
    old = split_field(field_ref, high_ref, low_ref, channels)
    for step in range(1, steps - 1):
        hear(step - 1)
        tell(step)
    total_ref[...] = jnp.zeros_like(total_ref)

    plane = lines * groups
    rounds = peers // BATCH
    early = groups
    new = jnp.zeros((channels, capacity), jnp.float32)
    for j in range(rounds):
        batch = range(BATCH * j, BATCH * (j + 1))
        for u in range(BATCH * (j - 1), BATCH * j):
            if 0 <= u < early and u != itself:
                answer(u).start()
        for u in batch:
            if u != itself:
                ask(u).wait_recv()
        blocks = [side(u) * groups + asker(u)[1] for u in batch]
        new = new + interpolate(asked, blocks, values, high_ref, low_ref, gathered_ref)
        if j == rounds // 2:
            hear(steps - 2)
            tell(steps - 1)
    new = jnp.sum(new, axis=1, keepdims=True)
    parts[0] = as_row(old, 0) + as_row(new, channels)
    returned[groups + grp] = values[groups + grp]
    plane_mass[line * groups + grp] = parts[0]
    far = sorted(range(1, plane), key=lambda i: -min(i // groups, lines - i // groups) * groups - min(i % groups, groups - i % groups))
    for i in far:
        plane_copy(i).start()
    for u in range(groups, 2 * groups):
        answer(u).start()
    settle(plane_mass, plane - 1, plane_got)
    parts[1] = jnp.sum(plane_mass[...], axis=0)
    hear(steps - 1)
    ring_mass[place] = parts[1]
    for i in sorted(range(1, ring), key=lambda i: -min(i, ring - i)):
        ring_copy(i).start()
    for u in range(2 * groups, peers):
        answer(u).start()

    def put(j, carry):
        for i in range(2):
            @pl.when(2 * j + i != itself)
            def _():
                answer(2 * j + i).wait_recv()

        blocks = [side(2 * j + i) * groups + owner(2 * j + i)[1] for i in range(2)]
        scatter(point_ref, blocks, returned, total_ref, masked_ref, elements)
        return carry

    lax.fori_loop(0, peers // 2, put, 0)
    settle(request_ref, others, ask_sent)
    settle(values, others, back_sent)
    settle(plane_mass, plane - 1, plane_sent)
    settle(ring_mass, ring - 1, ring_sent)
    settle(ring_mass, ring - 1, ring_got)
    masses = jnp.sum(ring_mass[...], axis=0)
    factor = as_column(masses, channels, 0) / as_column(masses, channels, channels)
    factor_ref[...] = jnp.broadcast_to(factor, factor_ref.shape)


def step(counts, order, elem, coords, field, channels, sizes):
    peers, capacity = elem.shape
    rows, elements = field.shape
    width = -(-elements // 256) * 256
    lines, ring, groups = sizes
    vmem, dma = pltpu.VMEM, pltpu.SemaphoreType.DMA
    blocks = vmem((peers, channels, capacity), jnp.float32)
    table = vmem((rows + 2 * channels, width), jnp.bfloat16)
    plane = lines * groups
    return pl.pallas_call(
        lambda *refs: step_kernel(sizes, *refs),
        out_shape=(
            jax.ShapeDtypeStruct((rows, width), jnp.float32),
            jax.ShapeDtypeStruct((channels, width), jnp.float32),
        ),
        in_specs=[pl.BlockSpec(memory_space=pltpu.HBM)] * 5,
        out_specs=(pl.BlockSpec(memory_space=pltpu.VMEM),) * 2,
        scratch_shapes=[
            pltpu.SMEM(counts.shape, jnp.int32),
            vmem((order.shape[0] + 8, 128), jnp.int32),
            vmem(elem.shape, jnp.int32),
            vmem(coords.shape, jnp.float32),
            vmem(field.shape, jnp.float32),
            vmem((peers, 4, capacity), jnp.float32),
            vmem((peers, capacity), jnp.int32),
            vmem((peers, 4, capacity), jnp.float32),
            blocks,
            blocks,
            table,
            table,
            vmem((rows + 2 * channels, BATCH * capacity), jnp.float32),
            vmem((2, rows, 2 * capacity), jnp.bfloat16),
            vmem((2, 1, 128), jnp.float32),
            vmem((plane, 1, 128), jnp.float32),
            vmem((ring, 1, 128), jnp.float32),
            dma((5,)),
            dma(()), dma((peers,)), dma(()), dma((peers,)),
            dma(()), dma(()), dma(()), dma(()),
            pltpu.SemaphoreType.REGULAR((8,)),
        ],
        compiler_params=pltpu.CompilerParams(
            collective_id=0, has_side_effects=True, vmem_limit_bytes=24 << 20
        ),
        name="step",
    )(*(pltpu.with_memory_space_constraint(x, pltpu.HBM) for x in (counts, order, elem, coords, field)))


def local(lines, tracers, send_counts, point_order, depart_elem, depart_coords):
    nodes, levels, species, elements = tracers.shape
    channels = levels * species
    groups, capacity = depart_elem.shape[-2:]
    peers = SIDES * groups
    total, factor = step(
        send_counts.reshape(1, peers),
        point_order.reshape(-1, 128),
        depart_elem.reshape(peers, capacity),
        depart_coords.reshape(2 * peers, capacity),
        tracers.reshape(nodes * channels, elements),
        channels,
        (lines, lax.axis_size("sfc") // lines, groups),
    )
    out = total.reshape(nodes, channels, -1)[:, :, :elements] * factor[None, :, :elements]
    return out.reshape(nodes, levels, species, elements)


def solution(mesh, lines=4):
    both = ("sfc", "grp")
    return jax.shard_map(
        lambda *args: local(lines, *args),
        mesh=mesh,
        in_specs=(
            P(None, None, None, both),
            P("sfc", "grp", None),
            P("sfc", "grp", None),
            P("sfc", "grp", None, None, None),
            P("sfc", "grp", None, None, None, None),
        ),
        out_specs=P(None, None, None, both),
        check_vma=False,
    )
```
